128 devices in a mesh: dp: 8 (over x, z_lo), rep: 16 (over z_hi, y, core).
Axes of the slice: x: 4, y: 4, z: 4 (z_hi: 2, z_lo: 2; z = z_hi * 2 + z_lo), core: 2. Of those that a mesh axis runs over, the one named last changes fastest.
Arguments:
- queries: bfloat16 [65536, 2048], P(('dp', 'rep')), may hold values from -32 to 32
- key_rows: bfloat16 [65536, 2048], P(('dp', 'rep')), may hold values from -32 to 32
- values: bfloat16 [65536, 2048], P(('dp', 'rep')), may hold values from -6 to 6
- upstream: bfloat16 [65536, 2048], P(('dp', 'rep')), may hold values from -24 to 24
- out_weight: bfloat16 [2048, 2048], P(('dp', 'rep')), may hold values from -0.125 to 0.125
- sample_ids: int32 [128, 512], P(('dp', 'rep')), may hold values from 0 to 3, as said below
Outputs:
- grad_queries: bfloat16 [65536, 2048], P(('dp', 'rep'))
- grad_keys: bfloat16 [65536, 2048], P(('dp', 'rep'))
- grad_values: bfloat16 [65536, 2048], P(('dp', 'rep'))
- grad_weight: float32 [2048, 2048], P(('dp', 'rep'))
The draws below stay inside these ranges and needn't reach their ends.
Inputs may be any that keep to these rules, and one draw needn't show every extreme that they name: `sample_ids`: within a row the ids never fall, every row starts with 0 and ends with 3, and the tokens of one sample are contiguous.
All inputs are finite; a program needn't handle non-finite values.
Results may differ from the reference program's by a relative error of at most 0.015.
Values may be sent and summed in bfloat16 or wider, within the bound.
A program may use at most 192 MiB of HBM per device.

```python
import math
import jax
import jax.numpy as jnp
from jax import lax

D = 2048
H = 16
DH = 128
HD = 2048
LEN = 512
NSEG = 4
SEQS = 128
TOKENS = 65536


def draw_queries(key, part):
    normal_part = jnp.clip(jax.random.normal(jax.random.fold_in(key, 11), (SEQS, LEN, H, DH), jnp.float32), -4.0, 4.0)
    normal_part = jnp.clip(normal_part, -32.0, 32.0)
    return normal_part.reshape(SEQS * LEN, H * DH).astype(jnp.bfloat16)


def draw_key_rows(key, part):
    normal_part = jnp.clip(jax.random.normal(jax.random.fold_in(key, 17), (SEQS, LEN, H, DH), jnp.float32), -4.0, 4.0)
    normal_part = jnp.clip(normal_part, -32.0, 32.0)
    return normal_part.reshape(SEQS * LEN, H * DH).astype(jnp.bfloat16)


def draw_sample_ids(key, part):
    cut_points = jax.random.randint(jax.random.fold_in(key, 29), (SEQS, NSEG - 1), LEN // 8, LEN - LEN // 8)
    positions = jnp.arange(LEN, dtype=jnp.int32)
    passed = (positions[None, :, None] >= cut_points[:, None, :]).astype(jnp.int32)
    return jnp.sum(passed, axis=2).astype(jnp.int32)


def with_spikes(array, own_key, source, target, parts, factor):
    def block_of(axis_at):
        return (jnp.arange(array.shape[axis_at]) // (array.shape[axis_at] // parts)).reshape((-1,) + (1,) * (array.ndim - 1 - axis_at))

    first = jax.random.permutation(own_key, parts)[block_of(target)]
    second = (block_of(target) + parts // 2) % parts
    return jnp.where((block_of(source) == first) | (block_of(source) == second), factor * array, array)


def shard_levels(rng, extent, shards, smallest, largest):
    level = 1.0
    for axis_at, parts in shards:
        draws = jax.random.uniform(jax.random.fold_in(jax.random.fold_in(rng, 6), axis_at), (parts,), jnp.float32, smallest / len(shards), largest / len(shards))
        level = level * jnp.repeat(jnp.exp(draws), extent[axis_at] // parts).reshape((-1,) + (1,) * (len(extent) - 1 - axis_at))
    return level


def bell_draw(stream_key, shape, scale, most, cuts=(), kind=jnp.bfloat16):
    result = scale * jax.random.normal(stream_key, shape, jnp.float32)
    if cuts:
        result = result * shard_levels(stream_key, shape, cuts, -0.22, 0.18)
    return jnp.clip(result, -most, most).astype(kind)


def gaussian_with(stream_key, extent, deviation, limit, pieces, heavy, kind=jnp.bfloat16):
    values = deviation * jax.random.normal(stream_key, extent, jnp.float32)
    if pieces:
        values = values * shard_levels(stream_key, extent, pieces, -0.22, 0.18)
    return jnp.clip(with_spikes(values, jax.random.fold_in(stream_key, 3), *heavy), -limit, limit).astype(kind)


def setup_inputs(seed: int = 0) -> dict:
    streams_of = jax.random.split(jax.random.key(seed), 7)
    return {
        "queries": draw_queries(jax.random.fold_in(streams_of[6], 71), 0),
        "key_rows": draw_key_rows(jax.random.fold_in(streams_of[6], 71), 0),
        "values": bell_draw(streams_of[2], (TOKENS, HD), 1.0, 6.0, ((0, 128),)),
        "upstream": gaussian_with(streams_of[3], (TOKENS, D), 1.0, 24.0, ((0, 128),), (0, 1, 128, 5.5)),
        "out_weight": bell_draw(streams_of[4], (D, HD), HD ** -0.5, 0.125, ((0, 128),)),
        "sample_ids": draw_sample_ids(jax.random.fold_in(streams_of[6], 71), 0),
    }


def sequence_pass(seq_block):
    query_block, key_block, value_block, grad_block, ids_row = seq_block
    scaling = 1.0 / math.sqrt(DH)
    query_wide = query_block.astype(jnp.float32)
    key_wide = key_block.astype(jnp.float32)
    value_wide = value_block.astype(jnp.float32)
    grad_wide = grad_block.astype(jnp.float32)
    positions = jnp.arange(LEN, dtype=jnp.int32)
    causal = positions[None, :] <= positions[:, None]
    allowed = jnp.logical_and(causal, ids_row[None, :] == ids_row[:, None])[None]
    scores = jnp.einsum('qhd,khd->hqk', query_wide, key_wide) * scaling
    masked = jnp.where(allowed, scores, -jnp.inf)
    row_max = lax.optimization_barrier(jnp.max(masked, axis=2, keepdims=True))
    raised = jnp.where(allowed, jnp.exp(masked - row_max), 0.0)
    probabilities = raised / lax.optimization_barrier(jnp.sum(raised, axis=2, keepdims=True))
    probs_low = lax.optimization_barrier(probabilities.astype(jnp.bfloat16)).astype(jnp.float32)
    attended = jnp.einsum('hqk,khd->qhd', probs_low, value_wide).astype(jnp.bfloat16)
    grad_values = jnp.einsum('hqk,qhd->khd', probs_low, grad_wide).astype(jnp.bfloat16)
    grad_probs = jnp.einsum('qhd,khd->hqk', grad_wide, value_wide)
    row_inner = lax.optimization_barrier(jnp.sum(probabilities * grad_probs, axis=2, keepdims=True))
    grad_scores = lax.optimization_barrier((probabilities * (grad_probs - row_inner)).astype(jnp.bfloat16)).astype(jnp.float32)
    grad_queries = (scaling * jnp.einsum('hqk,khd->qhd', grad_scores, key_wide)).astype(jnp.bfloat16)
    grad_keys = (scaling * jnp.einsum('hqk,qhd->khd', grad_scores, query_wide)).astype(jnp.bfloat16)
    return (attended, grad_queries, grad_keys, grad_values)

def reference(queries, key_rows, values, upstream, out_weight, sample_ids):
    grad_attended = jnp.dot(upstream, out_weight, preferred_element_type=jnp.float32).astype(jnp.bfloat16)
    grad_attended = lax.optimization_barrier(grad_attended)
    split_shape = (SEQS, LEN, H, DH)
    results = lax.map(sequence_pass, (queries.reshape(split_shape), key_rows.reshape(split_shape), values.reshape(split_shape), grad_attended.reshape(split_shape), sample_ids))
    attended, grad_queries, grad_keys, grad_values = [stacked.reshape(TOKENS, H * DH) for stacked in results]
    grad_weight = jnp.dot(upstream.T, attended, preferred_element_type=jnp.float32) / math.sqrt(TOKENS)
    return (grad_queries, grad_keys, grad_values, grad_weight)
```

```python
import functools
import math

import jax
import jax.numpy as jnp
from jax import lax
from jax.experimental import pallas as pl
from jax.experimental.pallas import tpu as pltpu
from jax.sharding import PartitionSpec as P

H = 16
DH = 128
LEN = 512
HALF = 256
D = 2048
HD = 2048
RING = 4
ROWS = 16
SCALING = 1.0 / math.sqrt(DH)
SCALE2 = SCALING * math.log2(math.e)
NEG = -1e30
ALL = ("dp", "rep")
F32 = jnp.float32
BF16 = jnp.bfloat16
MESH = pl.DeviceIdType.MESH
EVERY = slice(None)

NN = (((1,), (0,)), ((), ()))
NT = (((1,), (1,)), ((), ()))
TN = (((0,), (0,)), ((), ()))

ORDERS = (("x", "y", "z"), ("y", "z", "x"), ("z", "x", "y"))
BOUNDS = (0, 640, 1280, 2048)
CUTS = (384, 1024, 1664)


def dot(a, b, dims=NN):
    return lax.dot_general(a, b, dims, preferred_element_type=F32)


def fill_bias(ids, bias_a, bias_b):
    start = jnp.zeros((1, LEN), jnp.int32)
    for v in range(3):
        count = jnp.sum((ids == v).astype(jnp.int32), axis=1, keepdims=True)
        start = start + jnp.where(ids > v, count, 0)
    t = lax.broadcasted_iota(jnp.int32, (HALF, LEN), 1)
    u = lax.broadcasted_iota(jnp.int32, (HALF, LEN), 0)
    bias_a[...] = jnp.where((u >= start) & (u <= t), 0.0, NEG).astype(F32)
    t = lax.broadcasted_iota(jnp.int32, (HALF, HALF), 1) + HALF
    u = lax.broadcasted_iota(jnp.int32, (HALF, HALF), 0) + HALF
    bias_b[...] = jnp.where((u >= start[:, HALF:]) & (u <= t), 0.0, NEG).astype(F32)


def head_forward(q, k, v, bias_a, bias_b):
    xa = dot(k[:HALF], q, NT) * SCALE2 + bias_a[...]
    xb = dot(k[HALF:], q[HALF:], NT) * SCALE2 + bias_b[...]
    ma = jnp.max(xa, axis=0, keepdims=True)
    mb = jnp.maximum(ma[:, HALF:], jnp.max(xb, axis=0, keepdims=True))
    m = jnp.concatenate([ma[:, :HALF], mb], axis=1)
    ea = jnp.exp2(xa - m)
    eb = jnp.exp2(xb - mb)
    la = jnp.sum(ea, axis=0, keepdims=True)
    lb = la[:, HALF:] + jnp.sum(eb, axis=0, keepdims=True)
    inv = 1.0 / jnp.concatenate([la[:, :HALF], lb], axis=1)
    pa = (ea * inv).astype(BF16)
    pb = (eb * inv[:, HALF:]).astype(BF16)
    vt = v.T
    ot_a = dot(vt[:, :HALF], pa)
    ot_b = dot(vt[:, HALF:], pb)
    ot = jnp.concatenate([ot_a[:, :HALF], ot_a[:, HALF:] + ot_b], axis=1)
    return ot.astype(BF16).T, pa, pb


def head_backward(q, k, v, g, low_a, low_b):
    q1, g1 = q[HALF:], g[HALF:]
    dpa = dot(v[:HALF], g, NT)
    dpb = dot(v[HALF:], g1, NT)
    pa = low_a.astype(F32)
    pb = low_b.astype(F32)
    ia = jnp.sum(pa * dpa, axis=0, keepdims=True)
    ib = ia[:, HALF:] + jnp.sum(pb * dpb, axis=0, keepdims=True)
    inner = jnp.concatenate([ia[:, :HALF], ib], axis=1)
    dsa = (pa * (dpa - inner)).astype(BF16)
    dsb = (pb * (dpb - ib)).astype(BF16)
    gv = (dot(low_a, g).astype(BF16), dot(low_b, g1).astype(BF16))
    gk = ((dot(dsa, q) * SCALING).astype(BF16), (dot(dsb, q1) * SCALING).astype(BF16))
    kt = k.T
    qt_a = dot(kt[:, :HALF], dsa)
    qt_b = dot(kt[:, HALF:], dsb)
    qt = jnp.concatenate([qt_a[:, :HALF], qt_a[:, HALF:] + qt_b], axis=1)
    return (qt * SCALING).astype(BF16).T, gk, gv


def kernel(
    ids, q_hbm, k_hbm, v_hbm, up_hbm, w_hbm, gq_hbm, gk_hbm, gv_hbm, gw_out,
    q, k, v, up, w, gw, pair, r1, r2p, r2m, ga, att, prob_a, prob_b, bias_a, bias_b,
    load_sem, out_sem, send_sem, recv_sem,
):
    dp, rep = lax.axis_index("dp"), lax.axis_index("rep")
    core = lax.rem(rep, 2)
    own = {
        "x": dp // 2,
        "y": lax.rem(rep // 2, RING),
        "z": (rep // 8) * 2 + lax.rem(dp, 2),
    }

    def near(dim, shift):
        at = dict(own)
        at[dim] = lax.rem(own[dim] + shift + RING, RING)
        x, y, z = at["x"], at["y"], at["z"]
        return (x * 2 + lax.rem(z, 2), (z // 2) * 8 + y * 2 + core)

    sibling = (dp, rep + 1 - 2 * core)

    def step(dim, shift):
        return lax.rem(own[dim] + shift + RING, RING)

    def place(at):
        x, y = at.get("x", EVERY), at.get("y", EVERY)
        if "z" in at:
            return (x, lax.rem(at["z"], 2), at["z"] // 2, y)
        return (x, EVERY, EVERY, y)

    def cols(lo, hi):
        return pl.ds(lo, hi - lo)

    started = []

    def send(src, dst, device):
        n = len(started)
        copy = pltpu.make_async_remote_copy(
            src_ref=src, dst_ref=dst, send_sem=send_sem.at[n], recv_sem=recv_sem.at[n],
            device_id=device, device_id_type=MESH,
        )
        copy.start()
        started.append(copy)
        return copy

    def arrived(copies):
        for copy in copies:
            copy.wait_recv()

    here = place(own)
    w_load = pltpu.make_async_copy(w_hbm, w.at[(*here, core)], load_sem.at[0])
    w_load.start()
    loads = []
    for c in range(3):
        part = cols(BOUNDS[c], BOUNDS[c + 1])
        group = []
        for i, (src, dst) in enumerate(((q_hbm, q), (k_hbm, k), (v_hbm, v))):
            copy = pltpu.make_async_copy(
                src.at[:, part], dst.at[:, part], load_sem.at[1 + 3 * c + i]
            )
            copy.start()
            group.append(copy)
        loads.append(group)
    up_load = pltpu.make_async_copy(up_hbm, up, load_sem.at[10])
    up_load.start()

    barrier = pltpu.get_barrier_semaphore()
    peers = [near(d, s) for d in ("x", "y", "z") for s in (1, -1, 2)] + [sibling]
    for peer in peers:
        pl.semaphore_signal(barrier, inc=1, device_id=peer, device_id_type=MESH)
    fill_bias(ids[...], bias_a, bias_b)
    pl.semaphore_wait(barrier, len(peers))
    w_load.wait()

    def share(at, lo, hi, device):
        ref = w.at[(*place(at), core, EVERY, cols(lo, hi))]
        return send(ref, ref, device)

    def spec(c):
        return (*ORDERS[c], BOUNDS[c], CUTS[c], BOUNDS[c + 1])

    crossed = []

    def cross(at, lo, hi):
        crossed.append(share(at, lo, hi, sibling))

    first = []
    for c in range(3):
        a, b, d, lo, mid, hi = spec(c)
        first += [share(own, lo, hi, near(a, s)) for s in (1, -1, 2)]

    def forward_pairs(lo, hi):
        def body(i, _):
            for j in range(2):
                h = i * 2 + j
                at = pl.ds(pl.multiple_of(h * DH, DH), DH)
                o, pa, pb = head_forward(q[:, at], k[:, at], v[:, at], bias_a, bias_b)
                att[:, at] = o
                prob_a[h] = pa
                prob_b[h] = pb
            return 0

        lax.fori_loop(lo, hi, body, 0)

    def weight_partial(c):
        lo, hi = BOUNDS[c], BOUNDS[c + 1]

        def body(i, _):
            rows = pl.ds(pl.multiple_of(i * 256, 256), 256)
            block = dot(up[:, rows], att[:, lo:hi], TN).astype(BF16)
            gw[i // 2, lax.rem(i, 2), :, :, :, :, cols(lo, hi)] = block.reshape(
                2, RING, 2, ROWS, hi - lo
            )
            return 0

        lax.fori_loop(0, 8, body, 0)
        part = cols(lo, hi)
        return send(
            gw.at[:, :, :, :, 1 - core, :, part], pair.at[:, :, :, :, :, part], sibling
        )

    def add_pair(c, copy):
        part = cols(BOUNDS[c], BOUNDS[c + 1])
        arrived([copy])

        def body(i, _):
            mine = gw[i, :, :, :, core, :, part].astype(F32)
            gw[i, :, :, :, core, :, part] = (
                mine + pair[i, :, :, :, :, part].astype(F32)
            ).astype(BF16)
            return 0

        lax.fori_loop(0, RING, body, 0)

    def gwi(at, lo, hi):
        return (*place(at), core, EVERY, cols(lo, hi))

    def bufi(at, lo, hi):
        return (*place(at), EVERY, cols(lo, hi))

    def ring_start(c, d, at, shifted):
        lo, mid, hi = BOUNDS[c], CUTS[c], BOUNDS[c + 1]
        far, up1, down1 = step(d, 2), step(d, 1), step(d, -1)
        far_at, up_at, down_at = ({**at, d: i} for i in (far, up1, down1))
        up_to, down_to = ({**shifted, d: i} for i in (up1, down1))
        return (
            [
                send(gw.at[gwi(far_at, lo, mid)], r1.at[bufi(far_at, lo, mid)], near(d, 1)),
                send(gw.at[gwi(far_at, mid, hi)], r1.at[bufi(far_at, mid, hi)], near(d, -1)),
            ],
            [
                send(gw.at[gwi(up_at, mid, hi)], r2p.at[bufi(up_to, mid, hi)], near(d, 1)),
                send(gw.at[gwi(down_at, lo, mid)], r2m.at[bufi(down_to, lo, mid)], near(d, -1)),
            ],
        )

    def ring_middle(c, d, at, shifted, state):
        lo, mid, hi = BOUNDS[c], CUTS[c], BOUNDS[c + 1]
        relayed, direct = state
        arrived(relayed)
        done = list(direct)
        for shift, l, h, buf in ((1, lo, mid, r2p), (-1, mid, hi, r2m)):
            spot = {**at, d: step(d, shift)}
            to = {**shifted, d: step(d, shift)}
            src = gwi(spot, l, h)
            gw[src] = (gw[src].astype(F32) + r1[bufi(spot, l, h)].astype(F32)).astype(BF16)
            done.append(send(gw.at[src], buf.at[bufi(to, l, h)], near(d, shift)))
        return done

    def ring_end(c, d, at, shifted, copies):
        lo, hi = BOUNDS[c], BOUNDS[c + 1]
        arrived(copies)
        spot = gwi({**at, d: own[d]}, lo, hi)
        got = bufi({**shifted, d: own[d]}, lo, hi)
        gw[spot] = (
            gw[spot].astype(F32) + r2p[got].astype(F32) + r2m[got].astype(F32)
        ).astype(BF16)

    def places(c, ring):
        a, b, d = ORDERS[c]
        if ring == 0:
            return (c, d, {}, {})
        return (c, b, {d: own[d]}, {d: step(d, 1)})

    def last_start(c):
        a, b, d, lo, mid, hi = spec(c)
        copies = []
        for shift, buf in ((1, r1), (-1, r2p), (2, r2m)):
            at = {**own, a: step(a, shift)}
            to = {**at, d: step(d, 2)}
            copies.append(send(gw.at[gwi(at, lo, hi)], buf.at[bufi(to, lo, hi)], near(a, shift)))
        return copies

    def last_end(c, copies):
        a, b, d, lo, mid, hi = spec(c)
        arrived(copies)
        got = bufi({**own, d: step(d, 2)}, lo, hi)
        total = gw[gwi(own, lo, hi)].astype(F32)
        for buf in (r1, r2p, r2m):
            total = total + buf[got].astype(F32)
        gw_out[:, lo:hi] = total * (1.0 / 256.0)

    state = {}

    def gather_first():
        arrived(first)
        out = []
        for c in range(3):
            a, b, d, lo, mid, hi = spec(c)
            at = {b: own[b], d: own[d]}
            out += [share(at, lo, hi, near(b, s)) for s in (1, -1)]
        state["ring"] = out
        state["sub"] = {}
        for c in range(3):
            sub_start(c, 0)
        for c in range(3):
            a, b, d, lo, mid, hi = spec(c)
            cross({b: own[b], d: own[d]}, lo, hi)

    def sub_start(c, shift):
        a, b, d, lo, mid, hi = spec(c)
        at = {b: step(b, shift), d: own[d]}
        state["sub"][c, shift] = [share(at, lo, hi, near(d, s)) for s in (1, -1)]

    def sub_middle(c, shift):
        a, b, d, lo, mid, hi = spec(c)
        arrived(state["sub"][c, shift])
        at = {b: step(b, shift)}
        below, above = {**at, d: step(d, -1)}, {**at, d: step(d, 1)}
        state["sub"][c, shift] = [
            share(below, lo, mid, near(d, 1)), share(above, mid, hi, near(d, -1))
        ]
        cross(below, lo, hi)
        cross(above, lo, hi)

    def sub_end(c, shift):
        a, b, d, lo, mid, hi = spec(c)
        arrived(state["sub"][c, shift])
        cross({b: step(b, shift), d: step(d, 2)}, lo, hi)

    def gather_second():
        arrived(state["ring"])
        out = []
        for c in range(3):
            a, b, d, lo, mid, hi = spec(c)
            below, above = {b: step(b, -1), d: own[d]}, {b: step(b, 1), d: own[d]}
            out += [share(below, lo, mid, near(b, 1)), share(above, mid, hi, near(b, -1))]
        state["ring"] = out
        for c in range(3):
            sub_start(c, 1)
            sub_start(c, -1)
        for c in range(3):
            a, b, d, lo, mid, hi = spec(c)
            cross({b: step(b, -1), d: own[d]}, lo, hi)
            cross({b: step(b, 1), d: own[d]}, lo, hi)

    def gather_third():
        arrived(state["ring"])
        for c in range(3):
            sub_start(c, 2)
        for c in range(3):
            a, b, d, lo, mid, hi = spec(c)
            cross({b: step(b, 2), d: own[d]}, lo, hi)

    def for_subs(f, shifts):
        for shift in shifts:
            for c in range(3):
                f(c, shift)

    arrived_load = lambda group: [copy.wait() for copy in group]
    arrived_load(loads[0])
    forward_pairs(0, 2)
    gather_first()
    arrived_load(loads[1])
    forward_pairs(2, 3)
    up_load.wait()
    gather_second()
    pair0 = weight_partial(0)
    gather_third()
    for_subs(sub_middle, (0,))
    forward_pairs(3, 5)
    add_pair(0, pair0)
    p0, q0 = places(0, 0), places(0, 1)
    ring0 = ring_start(*p0)
    pair1 = weight_partial(1)
    for_subs(sub_middle, (1, -1))
    for_subs(sub_end, (0,))
    arrived_load(loads[2])
    forward_pairs(5, 8)
    for_subs(sub_middle, (2,))
    add_pair(1, pair1)
    p1, q1 = places(1, 0), places(1, 1)
    ring1 = ring_start(*p1)
    for_subs(sub_end, (1, -1))
    pair2 = weight_partial(2)
    ring0 = ring_middle(*p0, ring0)
    for_subs(sub_end, (2,))
    add_pair(2, pair2)
    p2, q2 = places(2, 0), places(2, 1)
    ring2 = ring_start(*p2)
    arrived(crossed)

    def attended_grads(i, _):
        at = pl.ds(pl.multiple_of(i * 256, 256), 256)
        block = w[:, :, :, :, :, :, at].reshape(D, 256)
        ga[:, at] = dot(up[...], block).astype(BF16)
        return 0

    def backward_heads(lo, hi):
        def body(h, _):
            at = pl.ds(pl.multiple_of(h * DH, DH), DH)
            dq, dk, dv = head_backward(q[:, at], k[:, at], v[:, at], ga[:, at], prob_a[h], prob_b[h])
            q[:, at] = dq
            for i in range(2):
                k[i * HALF : (i + 1) * HALF, at] = dk[i]
                v[i * HALF : (i + 1) * HALF, at] = dv[i]
            return 0

        lax.fori_loop(lo, hi, body, 0)
        for i, (src, dst) in enumerate(((q, gq_hbm), (k, gk_hbm), (v, gv_hbm))):
            part = cols(lo * DH, hi * DH)
            copy = pltpu.make_async_copy(src.at[:, part], dst.at[:, part], out_sem.at[len(outs)])
            copy.start()
            outs.append(copy)

    outs = []
    lax.fori_loop(0, 4, attended_grads, 0)
    ring1 = ring_middle(*p1, ring1)
    ring_end(*p0, ring0)
    ring0 = ring_start(*q0)
    lax.fori_loop(4, 8, attended_grads, 0)
    ring2 = ring_middle(*p2, ring2)
    backward_heads(0, 3)
    ring0 = ring_middle(*q0, ring0)
    ring_end(*p1, ring1)
    ring1 = ring_start(*q1)
    backward_heads(3, 6)
    ring_end(*q0, ring0)
    last0 = last_start(0)
    ring1 = ring_middle(*q1, ring1)
    ring_end(*p2, ring2)
    ring2 = ring_start(*q2)
    backward_heads(6, 9)
    ring_end(*q1, ring1)
    last1 = last_start(1)
    ring2 = ring_middle(*q2, ring2)
    last_end(0, last0)
    backward_heads(9, 12)
    ring_end(*q2, ring2)
    last2 = last_start(2)
    last_end(1, last1)
    backward_heads(12, 16)
    last_end(2, last2)
    for copy in outs:
        copy.wait()
    for copy in started:
        copy.wait_send()


COPIES = 176


def whole(q, k, v, up, w, ids):
    chips = (RING, 2, 2, RING)
    wide = jax.ShapeDtypeStruct((LEN, HD), BF16)
    any_spec = pl.BlockSpec(memory_space=pl.ANY)
    vmem_spec = pl.BlockSpec(memory_space=pltpu.VMEM)
    return pl.pallas_call(
        kernel,
        in_specs=[vmem_spec] + [any_spec] * 5,
        out_specs=[any_spec] * 3 + [vmem_spec],
        out_shape=[wide] * 3 + [jax.ShapeDtypeStruct((ROWS, HD), F32)],
        scratch_shapes=[pltpu.VMEM((LEN, HD), BF16)] * 4
        + [pltpu.VMEM((*chips, 2, ROWS, HD), BF16)] * 2
        + [pltpu.VMEM((*chips, ROWS, HD), BF16)] * 4
        + [pltpu.VMEM((LEN, HD), BF16)] * 2
        + [pltpu.VMEM((H, HALF, LEN), BF16), pltpu.VMEM((H, HALF, HALF), BF16)]
        + [pltpu.VMEM((HALF, LEN), F32), pltpu.VMEM((HALF, HALF), F32)]
        + [
            pltpu.SemaphoreType.DMA((11,)),
            pltpu.SemaphoreType.DMA((15,)),
            pltpu.SemaphoreType.DMA((COPIES,)),
            pltpu.SemaphoreType.DMA((COPIES,)),
        ],
        compiler_params=pltpu.CompilerParams(
            collective_id=0, has_side_effects=True, vmem_limit_bytes=67_000_000
        ),
        name="whole",
    )(ids, q, k, v, up, w)


def shards(queries, key_rows, values, upstream, out_weight, sample_ids):
    return tuple(whole(queries, key_rows, values, upstream, out_weight, sample_ids))


def solution(mesh):
    return jax.shard_map(
        shards,
        mesh=mesh,
        in_specs=(P(ALL, None),) * 6,
        out_specs=(P(ALL, None),) * 4,
        check_vma=False,
    )
```

```python
import functools
import math

import jax
import jax.numpy as jnp
from jax import lax
from jax.experimental import pallas as pl
from jax.experimental.pallas import tpu as pltpu
from jax.sharding import PartitionSpec as P

H = 16
DH = 128
LEN = 512
HALF = 256
D = 2048
HD = 2048
RING = 4
ROWS = 16
SCALING = 1.0 / math.sqrt(DH)
SCALE2 = SCALING * math.log2(math.e)
NEG = -1e30
ALL = ("dp", "rep")
F32 = jnp.float32
BF16 = jnp.bfloat16
MESH = pl.DeviceIdType.MESH
EVERY = slice(None)

NN = (((1,), (0,)), ((), ()))
NT = (((1,), (1,)), ((), ()))
TN = (((0,), (0,)), ((), ()))

ORDERS = (("x", "y", "z"), ("y", "z", "x"), ("z", "x", "y"))
CHUNKS = ((0, 256, 512, 768), (768, 1024, 1280, 1536), (1536, 1664, 1792, 2048))


def dot(a, b, dims=NN):
    return lax.dot_general(a, b, dims, preferred_element_type=F32)


def fill_bias(ids, bias_a, bias_b):
    start = jnp.zeros((1, LEN), jnp.int32)
    for v in range(3):
        count = jnp.sum((ids == v).astype(jnp.int32), axis=1, keepdims=True)
        start = start + jnp.where(ids > v, count, 0)
    t = lax.broadcasted_iota(jnp.int32, (HALF, LEN), 1)
    u = lax.broadcasted_iota(jnp.int32, (HALF, LEN), 0)
    bias_a[...] = jnp.where((u >= start) & (u <= t), 0.0, NEG).astype(F32)
    t = lax.broadcasted_iota(jnp.int32, (HALF, HALF), 1) + HALF
    u = lax.broadcasted_iota(jnp.int32, (HALF, HALF), 0) + HALF
    bias_b[...] = jnp.where((u >= start[:, HALF:]) & (u <= t), 0.0, NEG).astype(F32)


def head_forward(q, k, v, bias_a, bias_b):
    xa = dot(k[:HALF], q, NT) * SCALE2 + bias_a[...]
    xb = dot(k[HALF:], q[HALF:], NT) * SCALE2 + bias_b[...]
    ma = jnp.max(xa, axis=0, keepdims=True)
    mb = jnp.maximum(ma[:, HALF:], jnp.max(xb, axis=0, keepdims=True))
    m = jnp.concatenate([ma[:, :HALF], mb], axis=1)
    ea = jnp.exp2(xa - m)
    eb = jnp.exp2(xb - mb)
    la = jnp.sum(ea, axis=0, keepdims=True)
    lb = la[:, HALF:] + jnp.sum(eb, axis=0, keepdims=True)
    inv = 1.0 / jnp.concatenate([la[:, :HALF], lb], axis=1)
    pa = (ea * inv).astype(BF16)
    pb = (eb * inv[:, HALF:]).astype(BF16)
    vt = v.T
    ot_a = dot(vt[:, :HALF], pa)
    ot_b = dot(vt[:, HALF:], pb)
    ot = jnp.concatenate([ot_a[:, :HALF], ot_a[:, HALF:] + ot_b], axis=1)
    return ot.astype(BF16).T, pa, pb


def head_backward(q, k, v, g, low_a, low_b):
    q1, g1 = q[HALF:], g[HALF:]
    dpa = dot(v[:HALF], g, NT)
    dpb = dot(v[HALF:], g1, NT)
    pa = low_a.astype(F32)
    pb = low_b.astype(F32)
    ia = jnp.sum(pa * dpa, axis=0, keepdims=True)
    ib = ia[:, HALF:] + jnp.sum(pb * dpb, axis=0, keepdims=True)
    inner = jnp.concatenate([ia[:, :HALF], ib], axis=1)
    dsa = (pa * (dpa - inner)).astype(BF16)
    dsb = (pb * (dpb - ib)).astype(BF16)
    gv = (dot(low_a, g).astype(BF16), dot(low_b, g1).astype(BF16))
    gk = ((dot(dsa, q) * SCALING).astype(BF16), (dot(dsb, q1) * SCALING).astype(BF16))
    kt = k.T
    qt_a = dot(kt[:, :HALF], dsa)
    qt_b = dot(kt[:, HALF:], dsb)
    qt = jnp.concatenate([qt_a[:, :HALF], qt_a[:, HALF:] + qt_b], axis=1)
    return (qt * SCALING).astype(BF16).T, gk, gv


def kernel(
    ids_hbm, q_hbm, k_hbm, v_hbm, up_hbm, w_hbm,
    q, k, v, gw_out,
    up, w, gw, pair, r1, r2p, r2m, att, prob_a, prob_b, bias_a, bias_b,
    ids, load_sem, send_sem, recv_sem, plane_sem,
):
    dp, rep = lax.axis_index("dp"), lax.axis_index("rep")
    core = lax.rem(rep, 2)
    own = {
        "x": dp // 2,
        "y": lax.rem(rep // 2, RING),
        "z": (rep // 8) * 2 + lax.rem(dp, 2),
    }

    def away(shifts):
        x, y, z = (lax.rem(own[d] + shifts.get(d, 0) + RING, RING) for d in ("x", "y", "z"))
        return (x * 2 + lax.rem(z, 2), (z // 2) * 8 + y * 2 + core)

    def near(dim, shift):
        return away({dim: shift})

    sibling = (dp, rep + 1 - 2 * core)

    def step(dim, shift):
        return lax.rem(own[dim] + shift + RING, RING)

    def place(at):
        x, y = (
            pl.ds(2 * i[0], 2) if isinstance(i, tuple) else i
            for i in (at.get("x", EVERY), at.get("y", EVERY))
        )
        z = at.get("z", EVERY)
        if isinstance(z, tuple):
            return (x, EVERY, z[0], y)
        if z is EVERY:
            return (x, EVERY, EVERY, y)
        return (x, lax.rem(z, 2), z // 2, y)

    def cols(lo, hi):
        return pl.ds(lo, hi - lo)

    groups = []

    def blob(k, part):
        lead = {
            3: (0, 0, 0, pl.ds(0, 3)),
            12: (pl.ds(0, 3), 0, 0, EVERY),
            16: (0, EVERY, EVERY, EVERY),
            32: (pl.ds(0, 2), EVERY, EVERY, EVERY),
            64: (EVERY, EVERY, EVERY, EVERY),
        }[k]
        return pair.at[(*lead, EVERY, part)]

    def group(k, n):
        groups.append(blob(k, chunk(n)))
        return len(groups) - 1

    def send(g, src, dst, device):
        pltpu.make_async_remote_copy(
            src_ref=src, dst_ref=dst, send_sem=send_sem.at[g], recv_sem=recv_sem.at[g],
            device_id=device, device_id_type=MESH,
        ).start()

    def arrived(g):
        pltpu.make_async_copy(groups[g], groups[g], recv_sem.at[g]).wait()

    def sent(g):
        pltpu.make_async_copy(groups[g], groups[g], send_sem.at[g]).wait()

    def chunk(n):
        return cols(CHUNKS[n][0], CHUNKS[n][3])

    def piece(n, c):
        return cols(CHUNKS[n][c], CHUNKS[n][c + 1])

    here = place(own)
    w_load = pltpu.make_async_copy(w_hbm, w.at[(*here, core)], load_sem.at[0])
    w_load.start()
    ids_load = pltpu.make_async_copy(ids_hbm, ids, load_sem.at[11])
    ids_load.start()
    loads = []
    for c in range(3):
        part = cols(CHUNKS[c][0], CHUNKS[c][3])
        trio = []
        for i, (src, dst) in enumerate(((q_hbm, q), (k_hbm, k), (v_hbm, v))):
            copy = pltpu.make_async_copy(
                src.at[:, part], dst.at[:, part], load_sem.at[1 + 3 * c + i]
            )
            copy.start()
            trio.append(copy)
        loads.append(trio)
    up_load = pltpu.make_async_copy(up_hbm, up, load_sem.at[10])
    up_load.start()

    barrier = pltpu.get_barrier_semaphore()
    beside = [near(d, s) for d in ("x", "y", "z") for s in (1, -1, 2)]
    peers = beside + [sibling]
    for peer in peers:
        pl.semaphore_signal(barrier, inc=1, device_id=peer, device_id_type=MESH)
    ids_load.wait()
    fill_bias(ids[...], bias_a, bias_b)
    pl.semaphore_wait(barrier, len(peers))
    w_load.wait()

    def share(g, at, part, device):
        ref = w.at[(*place(at), core, EVERY, part)]
        send(g, ref, ref, device)

    crossed = [group(64, n) for n in range(3)]
    row = [group(3, n) for n in range(3)]
    rest = [group(12, n) for n in range(3)]
    wide = [group(32, n) for n in range(3)]
    relay = [group(16, n) for n in range(3)]

    def cross(n, c, at):
        share(crossed[n], at, piece(n, c), sibling)

    def spread(n, shifts):
        for shift in shifts:
            for c in range(3):
                a, b, d = ORDERS[c]
                at = {b: step(b, shift), d: own[d]}
                for s in (1, -1):
                    share(wide[n], at, piece(n, c), near(d, s))

    def gather_a(n):
        arrived(row[n])
        spread(n, (0,))

    def gather_b(n):
        arrived(rest[n])
        spread(n, (1, -1, 2))
        for c in range(3):
            d = ORDERS[c][2]
            cross(n, c, {d: own[d]})

    def gather_d(n):
        arrived(wide[n])
        for c in range(3):
            a, b, d = ORDERS[c]
            for s, half in ((1, 0), (-1, 1)):
                share(relay[n], {b: (half,), d: step(d, -s)}, piece(n, c), near(d, s))
        for c in range(3):
            d = ORDERS[c][2]
            for s in (1, -1):
                cross(n, c, {d: step(d, s)})

    def gather_e(n):
        arrived(relay[n])
        for c in range(3):
            d = ORDERS[c][2]
            cross(n, c, {d: step(d, 2)})

    for n in range(3):
        for c in range(3):
            a, b, d = ORDERS[c]
            for s in (1, -1, 2):
                share(row[n], own, piece(n, c), near(a, s))
    for peer in beside:
        pl.semaphore_signal(plane_sem, inc=1, device_id=peer, device_id_type=MESH)

    def gather_rest():
        pl.semaphore_wait(plane_sem, len(beside))
        for n in range(3):
            for c in range(3):
                a, b, d = ORDERS[c]
                for sb in (1, -1, 2):
                    for sa in (0, 1, -1, 2):
                        share(rest[n], own, piece(n, c), away({a: sa, b: sb}))

    def forward_pairs(lo, hi):
        def body(i, _):
            for j in range(2):
                h = i * 2 + j
                at = pl.ds(pl.multiple_of(h * DH, DH), DH)
                o, pa, pb = head_forward(q[:, at], k[:, at], v[:, at], bias_a, bias_b)
                att[:, at] = o
                prob_a[h] = pa
                prob_b[h] = pb
            return 0

        lax.fori_loop(lo, hi, body, 0)

    def weight_partial(n, lo_i, hi_i):
        lo, hi = CHUNKS[n][0], CHUNKS[n][3]

        def body(i, _):
            rows = pl.ds(pl.multiple_of(i * 256, 256), 256)
            block = dot(up[:, rows], att[:, lo:hi], TN).astype(BF16)
            gw[i // 2, lax.rem(i, 2), :, :, :, :, cols(lo, hi)] = block.reshape(
                2, RING, 2, ROWS, hi - lo
            )
            return 0

        lax.fori_loop(lo_i, hi_i, body, 0)

    swaps, pairs = {}, {}

    def swap_pair(n, half):
        g = group(32, n)
        swaps[n, half] = g
        part, x = chunk(n), pl.ds(2 * half, 2)
        send(g, gw.at[x, :, :, :, 1 - core, :, part], pair.at[x, :, :, :, :, part], sibling)

    def add_pair(n):
        part = chunk(n)

        def body(i, _):
            mine = gw[i, :, :, :, core, :, part].astype(F32)
            gw[i, :, :, :, core, :, part] = (
                mine + pair[i, :, :, :, :, part].astype(F32)
            ).astype(BF16)
            return 0

        for half in range(2):
            arrived(swaps[n, half])
            lax.fori_loop(2 * half, 2 * half + 2, body, 0)

    def gwi(at, part):
        return (*place(at), core, EVERY, part)

    def bufi(at, part):
        return (*place(at), EVERY, part)

    rings = {}
    SIDES = ((1, 0, r2p), (-1, 1, r2m))

    def start(n):
        rings[n] = (group(16, n), group(32, n))
        for c in range(3):
            a, b, d = ORDERS[c]
            part = piece(n, c)
            for shift, half, buf in SIDES:
                far = {d: step(d, 2), b: (half,)}
                send(rings[n][0], gw.at[gwi(far, part)], r1.at[bufi(far, part)], near(d, shift))
        for c in range(3):
            a, b, d = ORDERS[c]
            part = piece(n, c)
            for shift, half, buf in SIDES:
                tail = {d: step(d, shift), b: (1 - half,)}
                send(rings[n][1], gw.at[gwi(tail, part)], buf.at[bufi(tail, part)], near(d, shift))

    def middle(n):
        arrived(rings[n][0])
        for c in range(3):
            a, b, d = ORDERS[c]
            part = piece(n, c)
            for shift, half, buf in SIDES:
                tail = {d: step(d, shift), b: (half,)}
                src = gwi(tail, part)
                gw[src] = (
                    gw[src].astype(F32) + r1[bufi(tail, part)].astype(F32)
                ).astype(BF16)
        for c in range(3):
            a, b, d = ORDERS[c]
            part = piece(n, c)
            for shift, half, buf in SIDES:
                tail = {d: step(d, shift), b: (half,)}
                send(rings[n][1], gw.at[gwi(tail, part)], buf.at[bufi(tail, part)], near(d, shift))

    def end(n):
        arrived(rings[n][1])
        for c in range(3):
            d = ORDERS[c][2]
            part = piece(n, c)
            spot, got = gwi({d: own[d]}, part), bufi({d: own[d]}, part)
            gw[spot] = (
                gw[spot].astype(F32) + r2p[got].astype(F32) + r2m[got].astype(F32)
            ).astype(BF16)

    OTHERS = [(sa, sb) for sb in (2, 1, -1, 0) for sa in (2, 1, -1, 0) if (sa, sb) != (0, 0)]

    def plane_start(n):
        rings[n] = (group(12, n), group(3, n))
        for i, (sa, sb) in enumerate(OTHERS):
            for c in range(3):
                a, b, d = ORDERS[c]
                part = piece(n, c)
                src = gw.at[gwi({**own, a: step(a, sa), b: step(b, sb)}, part)]
                dst = r1.at[bufi({**own, d: step(d, 2)}, part)]
                send(rings[n][i // 12], src, dst, away({a: sa, b: sb}))

    def plane_end(n):
        arrived(rings[n][0])
        arrived(rings[n][1])
        for c in range(3):
            a, b, d = ORDERS[c]
            part = piece(n, c)
            total = gw[gwi(own, part)].astype(F32)
            for sa, sb in OTHERS:
                at = {a: step(a, sa), b: step(b, sb), d: step(d, 2)}
                total = total + r1[bufi(at, part)].astype(F32)
            gw_out[:, part] = total * (1.0 / 256.0)

    def attended_grads_part(n):
        lax.fori_loop(CHUNKS[n][0] // 256, CHUNKS[n][3] // 256, attended_grads, 0)

    def attended_grads(i, _):
        at = pl.ds(pl.multiple_of(i * 256, 256), 256)
        block = w[:, :, :, :, :, :, at].reshape(D, 256)
        att[:, at] = dot(up[...], block).astype(BF16)
        return 0

    def backward_heads(lo, hi):
        def body(h, _):
            at = pl.ds(pl.multiple_of(h * DH, DH), DH)
            dq, dk, dv = head_backward(q[:, at], k[:, at], v[:, at], att[:, at], prob_a[h], prob_b[h])
            q[:, at] = dq
            for i in range(2):
                k[i * HALF : (i + 1) * HALF, at] = dk[i]
                v[i * HALF : (i + 1) * HALF, at] = dv[i]
            return 0

        lax.fori_loop(lo, hi, body, 0)

    def loaded(trio):
        for copy in trio:
            copy.wait()

    loaded(loads[0])
    forward_pairs(0, 2)
    gather_rest()
    forward_pairs(2, 3)
    up_load.wait()
    gather_a(0)
    gather_a(1)
    gather_a(2)
    weight_partial(0, 0, 4)
    swap_pair(0, 0)
    weight_partial(0, 4, 8)
    swap_pair(0, 1)
    loaded(loads[1])
    forward_pairs(3, 6)
    add_pair(0)
    gather_b(0)
    weight_partial(1, 0, 4)
    swap_pair(1, 0)
    gather_b(1)
    weight_partial(1, 4, 8)
    swap_pair(1, 1)
    gather_b(2)
    start(0)
    loaded(loads[2])
    forward_pairs(6, 7)
    gather_d(0)
    forward_pairs(7, 8)
    add_pair(1)
    start(1)
    weight_partial(2, 0, 4)
    swap_pair(2, 0)
    gather_d(1)
    weight_partial(2, 4, 8)
    swap_pair(2, 1)
    gather_d(2)
    gather_e(0)
    middle(0)
    arrived(crossed[0])
    attended_grads_part(0)
    add_pair(2)
    start(2)
    gather_e(1)
    middle(1)
    backward_heads(0, 2)
    end(0)
    gather_e(2)
    backward_heads(2, 4)
    middle(2)
    plane_start(0)
    backward_heads(4, 6)
    end(1)
    plane_start(1)
    arrived(crossed[1])
    attended_grads_part(1)
    end(2)
    plane_start(2)
    backward_heads(6, 9)
    plane_end(0)
    backward_heads(9, 12)
    arrived(crossed[2])
    attended_grads_part(2)
    backward_heads(12, 14)
    plane_end(1)
    backward_heads(14, 16)
    plane_end(2)
    for g in range(len(groups)):
        sent(g)


GROUPS = 36


def whole(q, k, v, up, w, ids):
    chips = (RING, 2, 2, RING)
    wide = jax.ShapeDtypeStruct((LEN, HD), BF16)
    hbm_spec = pl.BlockSpec(memory_space=pltpu.HBM)
    vmem_spec = pl.BlockSpec(memory_space=pltpu.VMEM)
    return pl.pallas_call(
        kernel,
        in_specs=[hbm_spec] * 6,
        out_specs=[vmem_spec] * 4,
        out_shape=[wide] * 3 + [jax.ShapeDtypeStruct((ROWS, HD), F32)],
        scratch_shapes=[pltpu.VMEM((LEN, HD), BF16)]
        + [pltpu.VMEM((*chips, 2, ROWS, HD), BF16)] * 2
        + [pltpu.VMEM((*chips, ROWS, HD), BF16)] * 4
        + [pltpu.VMEM((LEN, HD), BF16)]
        + [pltpu.VMEM((H, HALF, LEN), BF16), pltpu.VMEM((H, HALF, HALF), BF16)]
        + [pltpu.VMEM((HALF, LEN), F32), pltpu.VMEM((HALF, HALF), F32)]
        + [
            pltpu.VMEM((1, LEN), jnp.int32),
            pltpu.SemaphoreType.DMA((12,)),
            pltpu.SemaphoreType.DMA((GROUPS,)),
            pltpu.SemaphoreType.DMA((GROUPS,)),
            pltpu.SemaphoreType.REGULAR,
        ],
        compiler_params=pltpu.CompilerParams(
            collective_id=0, has_side_effects=True, vmem_limit_bytes=49_000_000
        ),
        name="whole",
    )(ids, q, k, v, up, w)


def pass_on_kernel(*refs):
    held, results, sems = refs[:4], refs[4:8], refs[8]
    copies = [
        pltpu.make_async_copy(src, dst, sems.at[i])
        for i, (src, dst) in enumerate(zip(held, results))
    ]
    for copy in copies:
        copy.start()
    for copy in copies:
        copy.wait()


def pass_on(*arrays):
    return pl.pallas_call(
        pass_on_kernel,
        in_specs=[pl.BlockSpec(memory_space=pltpu.VMEM)] * 4,
        out_specs=[pl.BlockSpec(memory_space=pltpu.HBM)] * 4,
        out_shape=[jax.ShapeDtypeStruct(a.shape, a.dtype) for a in arrays],
        scratch_shapes=[pltpu.SemaphoreType.DMA((4,))],
        compiler_params=pltpu.CompilerParams(vmem_limit_bytes=8_000_000),
        name="pass_on",
    )(*arrays)


def shards(queries, key_rows, values, upstream, out_weight, sample_ids):
    return tuple(pass_on(*whole(queries, key_rows, values, upstream, out_weight, sample_ids)))


def solution(mesh):
    return jax.shard_map(
        shards,
        mesh=mesh,
        in_specs=(P(ALL, None),) * 6,
        out_specs=(P(ALL, None),) * 4,
        check_vma=False,
    )
```

```python
import functools
import math

import jax
import jax.numpy as jnp
from jax import lax
from jax.experimental import pallas as pl
from jax.experimental.pallas import tpu as pltpu
from jax.sharding import PartitionSpec as P

H = 16
DH = 128
LEN = 512
HALF = 256
D = 2048
HD = 2048
RING = 4
ROWS = 16
SCALING = 1.0 / math.sqrt(DH)
SCALE2 = SCALING * math.log2(math.e)
NEG = -1e30
ALL = ("dp", "rep")
F32 = jnp.float32
BF16 = jnp.bfloat16
MESH = pl.DeviceIdType.MESH
EVERY = slice(None)

NN = (((1,), (0,)), ((), ()))
NT = (((1,), (1,)), ((), ()))
TN = (((0,), (0,)), ((), ()))

ORDERS = (("x", "y", "z"), ("y", "z", "x"), ("z", "x", "y"))
CHUNKS = ((0, 256, 512, 768), (768, 1024, 1280, 1536), (1536, 1664, 1792, 2048))


def dot(a, b, dims=NN):
    return lax.dot_general(a, b, dims, preferred_element_type=F32)


def fill_bias(ids, bias_a, bias_b):
    start = jnp.zeros((1, LEN), jnp.int32)
    for v in range(3):
        count = jnp.sum((ids == v).astype(jnp.int32), axis=1, keepdims=True)
        start = start + jnp.where(ids > v, count, 0)
    t = lax.broadcasted_iota(jnp.int32, (HALF, LEN), 1)
    u = lax.broadcasted_iota(jnp.int32, (HALF, LEN), 0)
    bias_a[...] = jnp.where((u >= start) & (u <= t), 0.0, NEG).astype(F32)
    t = lax.broadcasted_iota(jnp.int32, (HALF, HALF), 1) + HALF
    u = lax.broadcasted_iota(jnp.int32, (HALF, HALF), 0) + HALF
    bias_b[...] = jnp.where((u >= start[:, HALF:]) & (u <= t), 0.0, NEG).astype(F32)


def head_forward(q, k, v, bias_a, bias_b):
    xa = dot(k[:HALF], q, NT) * SCALE2 + bias_a[...]
    xb = dot(k[HALF:], q[HALF:], NT) * SCALE2 + bias_b[...]
    ma = jnp.max(xa, axis=0, keepdims=True)
    mb = jnp.maximum(ma[:, HALF:], jnp.max(xb, axis=0, keepdims=True))
    m = jnp.concatenate([ma[:, :HALF], mb], axis=1)
    ea = jnp.exp2(xa - m)
    eb = jnp.exp2(xb - mb)
    la = jnp.sum(ea, axis=0, keepdims=True)
    lb = la[:, HALF:] + jnp.sum(eb, axis=0, keepdims=True)
    inv = 1.0 / jnp.concatenate([la[:, :HALF], lb], axis=1)
    pa = (ea * inv).astype(BF16)
    pb = (eb * inv[:, HALF:]).astype(BF16)
    vt = v.T
    ot_a = dot(vt[:, :HALF], pa)
    ot_b = dot(vt[:, HALF:], pb)
    ot = jnp.concatenate([ot_a[:, :HALF], ot_a[:, HALF:] + ot_b], axis=1)
    return ot.astype(BF16).T, pa, pb


def head_backward(q, k, v, g, low_a, low_b):
    q1, g1 = q[HALF:], g[HALF:]
    dpa = dot(v[:HALF], g, NT)
    dpb = dot(v[HALF:], g1, NT)
    pa = low_a.astype(F32)
    pb = low_b.astype(F32)
    ia = jnp.sum(pa * dpa, axis=0, keepdims=True)
    ib = ia[:, HALF:] + jnp.sum(pb * dpb, axis=0, keepdims=True)
    inner = jnp.concatenate([ia[:, :HALF], ib], axis=1)
    dsa = (pa * (dpa - inner)).astype(BF16)
    dsb = (pb * (dpb - ib)).astype(BF16)
    gv = (dot(low_a, g).astype(BF16), dot(low_b, g1).astype(BF16))
    gk = ((dot(dsa, q) * SCALING).astype(BF16), (dot(dsb, q1) * SCALING).astype(BF16))
    kt = k.T
    qt_a = dot(kt[:, :HALF], dsa)
    qt_b = dot(kt[:, HALF:], dsb)
    qt = jnp.concatenate([qt_a[:, :HALF], qt_a[:, HALF:] + qt_b], axis=1)
    return (qt * SCALING).astype(BF16).T, gk, gv


def kernel(
    ids_hbm, q_hbm, k_hbm, v_hbm, up_hbm, w_hbm,
    q, k, v, gw_out,
    up, up_t, w, gw, pair, r1, r2p, r2m, att, prob_a, prob_b, bias_a, bias_b,
    ids, load_sem, send_sem, recv_sem, plane_sem,
):
    dp, rep = lax.axis_index("dp"), lax.axis_index("rep")
    core = lax.rem(rep, 2)
    own = {
        "x": dp // 2,
        "y": lax.rem(rep // 2, RING),
        "z": (rep // 8) * 2 + lax.rem(dp, 2),
    }

    def away(shifts):
        x, y, z = (lax.rem(own[d] + shifts.get(d, 0) + RING, RING) for d in ("x", "y", "z"))
        return (x * 2 + lax.rem(z, 2), (z // 2) * 8 + y * 2 + core)

    def near(dim, shift):
        return away({dim: shift})

    sibling = (dp, rep + 1 - 2 * core)

    def step(dim, shift):
        return lax.rem(own[dim] + shift + RING, RING)

    def place(at):
        x, y = (
            pl.ds(2 * i[0], 2) if isinstance(i, tuple) else i
            for i in (at.get("x", EVERY), at.get("y", EVERY))
        )
        z = at.get("z", EVERY)
        if isinstance(z, tuple):
            return (x, EVERY, z[0], y)
        if z is EVERY:
            return (x, EVERY, EVERY, y)
        return (x, lax.rem(z, 2), z // 2, y)

    def cols(lo, hi):
        return pl.ds(lo, hi - lo)

    groups = []

    def blob(k, part):
        lead = {
            3: (0, 0, 0, pl.ds(0, 3)),
            4: (0, 0, 0, EVERY),
            8: (0, 0, EVERY, EVERY),
            12: (pl.ds(0, 3), 0, 0, EVERY),
            16: (0, EVERY, EVERY, EVERY),
            32: (pl.ds(0, 2), EVERY, EVERY, EVERY),
            64: (EVERY, EVERY, EVERY, EVERY),
        }[k]
        return pair.at[(*lead, EVERY, part)]

    def group(k, n):
        groups.append(blob(k, chunk(n)))
        return len(groups) - 1

    def send(g, src, dst, device):
        pltpu.make_async_remote_copy(
            src_ref=src, dst_ref=dst, send_sem=send_sem.at[g], recv_sem=recv_sem.at[g],
            device_id=device, device_id_type=MESH,
        ).start()

    def arrived(g):
        pltpu.make_async_copy(groups[g], groups[g], recv_sem.at[g]).wait()

    def sent(g):
        pltpu.make_async_copy(groups[g], groups[g], send_sem.at[g]).wait()

    def chunk(n):
        return cols(CHUNKS[n][0], CHUNKS[n][3])

    def piece(n, c):
        return cols(CHUNKS[n][c], CHUNKS[n][c + 1])

    barrier = pltpu.get_barrier_semaphore()
    beside = [near(d, s) for d in ("x", "y", "z") for s in (1, -1, 2)]
    peers = beside + [sibling]
    for peer in peers:
        pl.semaphore_signal(barrier, inc=1, device_id=peer, device_id_type=MESH)
    here = place(own)
    w_load = pltpu.make_async_copy(w_hbm, w.at[(*here, core)], load_sem.at[0])
    w_load.start()
    ids_load = pltpu.make_async_copy(ids_hbm, ids, load_sem.at[11])
    ids_load.start()
    loads = []
    for c in range(3):
        part = cols(CHUNKS[c][0], CHUNKS[c][3])
        trio = []
        for i, (src, dst) in enumerate(((q_hbm, q), (k_hbm, k), (v_hbm, v))):
            copy = pltpu.make_async_copy(
                src.at[:, part], dst.at[:, part], load_sem.at[1 + 3 * c + i]
            )
            copy.start()
            trio.append(copy)
        loads.append(trio)
    up_load = pltpu.make_async_copy(up_hbm, up, load_sem.at[10])
    up_load.start()

    pl.semaphore_wait(barrier, len(peers))
    w_load.wait()

    def share(g, at, part, device):
        ref = w.at[(*place(at), core, EVERY, part)]
        send(g, ref, ref, device)

    crossed = [group(64, n) for n in range(3)]
    gather = {}

    def cross(n, c, at):
        share(crossed[n], at, piece(n, c), sibling)

    def gather_start(n):
        gather[n] = group(3, n)
        for c in range(3):
            a, b, d = ORDERS[c]
            for s in (1, -1, 2):
                share(gather[n], own, piece(n, c), near(a, s))

    def gather_a(n):
        arrived(gather[n])
        gather[n] = group(8, n)
        for c in range(3):
            a, b, d = ORDERS[c]
            for s in (1, -1):
                share(gather[n], {b: own[b], d: own[d]}, piece(n, c), near(b, s))

    def gather_b(n):
        arrived(gather[n])
        gather[n] = group(4, n)
        for c in range(3):
            a, b, d = ORDERS[c]
            for s, half in ((1, 0), (-1, 1)):
                at = {a: (half,), b: step(b, -s), d: own[d]}
                share(gather[n], at, piece(n, c), near(b, s))

    def gather_c(n):
        arrived(gather[n])
        spread(n, (2,))
        for c in range(3):
            d = ORDERS[c][2]
            cross(n, c, {d: own[d]})

    def gather_d(n):
        arrived(wide[n])
        gather[n] = group(16, n)
        for c in range(3):
            a, b, d = ORDERS[c]
            for s, half in ((1, 0), (-1, 1)):
                share(gather[n], {b: (half,), d: step(d, -s)}, piece(n, c), near(d, s))
        for c in range(3):
            d = ORDERS[c][2]
            for s in (1, -1):
                cross(n, c, {d: step(d, s)})

    def gather_e(n):
        arrived(gather[n])
        for c in range(3):
            d = ORDERS[c][2]
            cross(n, c, {d: step(d, 2)})

    wide = [group(32, n) for n in range(3)]

    def spread(n, shifts):
        for shift in shifts:
            for c in range(3):
                a, b, d = ORDERS[c]
                at = {b: step(b, shift), d: own[d]}
                for s in (1, -1):
                    share(wide[n], at, piece(n, c), near(d, s))

    for n in range(3):
        gather_start(n)

    for peer in beside:
        pl.semaphore_signal(plane_sem, inc=1, device_id=peer, device_id_type=MESH)

    ids_load.wait()
    fill_bias(ids[...], bias_a, bias_b)

    def forward_pairs(lo, hi):
        def body(i, _):
            done = []
            for j in range(2):
                h = i * 2 + j
                at = pl.ds(pl.multiple_of(h * DH, DH), DH)
                done.append((h, at, head_forward(q[:, at], k[:, at], v[:, at], bias_a, bias_b)))
            for h, at, (o, pa, pb) in done:
                att[:, at] = o
                prob_a[h] = pa
                prob_b[h] = pb
            return 0

        lax.fori_loop(lo, hi, body, 0)

    def weight_partial(n, lo_i, hi_i):
        lo, hi = CHUNKS[n][0], CHUNKS[n][3]

        def body(i, _):
            rows = pl.ds(pl.multiple_of(i * 512, 512), 512)
            if n == 0:
                up_t[rows, :] = up[:, rows].T
            block = dot(up_t[rows, :], att[:, lo:hi]).astype(BF16)
            gw[i, :, :, :, :, :, cols(lo, hi)] = block.reshape(2, 2, RING, 2, ROWS, hi - lo)
            return 0

        lax.fori_loop(lo_i, hi_i, body, 0)

    swaps = {}

    def swap_pair(n, half):
        g = group(32, n)
        swaps[n, half] = g
        part, x = chunk(n), pl.ds(2 * half, 2)
        send(g, gw.at[x, :, :, :, 1 - core, :, part], pair.at[x, :, :, :, :, part], sibling)

    def add_pair(n):
        part = chunk(n)

        def body(i, _):
            mine = gw[i, :, :, :, core, :, part].astype(F32)
            gw[i, :, :, :, core, :, part] = (
                mine + pair[i, :, :, :, :, part].astype(F32)
            ).astype(BF16)
            return 0

        for half in range(2):
            arrived(swaps[n, half])
            lax.fori_loop(2 * half, 2 * half + 2, body, 0)

    def gwi(at, part):
        return (*place(at), core, EVERY, part)

    def bufi(at, part):
        return (*place(at), EVERY, part)

    def flow(n, c, ring):
        a, b, d = ORDERS[c]
        if ring == 0:
            return (d, b, {}, {}, piece(n, c))
        return (b, a, {d: own[d]}, {d: step(d, 1)}, piece(n, c))

    rings = {}
    SIDES = ((1, 0, r2p), (-1, 1, r2m))

    def start(n, ring):
        relayed, direct = group(4 if ring else 16, n), group(8 if ring else 32, n)
        rings[n] = (relayed, direct)
        for c in range(3):
            d, nxt, at, shifted, part = flow(n, c, ring)
            for shift, half, buf in SIDES:
                far = {**at, d: step(d, 2), nxt: (half,)}
                send(relayed, gw.at[gwi(far, part)], r1.at[bufi(far, part)], near(d, shift))
        for c in range(3):
            d, nxt, at, shifted, part = flow(n, c, ring)
            for shift, half, buf in SIDES:
                tail = {d: step(d, shift), nxt: (1 - half,)}
                src = gw.at[gwi({**at, **tail}, part)]
                send(direct, src, buf.at[bufi({**shifted, **tail}, part)], near(d, shift))

    def middle(n, ring):
        relayed, direct = rings[n]
        arrived(relayed)
        for c in range(3):
            d, nxt, at, shifted, part = flow(n, c, ring)
            for shift, half, buf in SIDES:
                tail = {d: step(d, shift), nxt: (half,)}
                src = gwi({**at, **tail}, part)
                gw[src] = (
                    gw[src].astype(F32) + r1[bufi({**at, **tail}, part)].astype(F32)
                ).astype(BF16)
        for c in range(3):
            d, nxt, at, shifted, part = flow(n, c, ring)
            for shift, half, buf in SIDES:
                tail = {d: step(d, shift), nxt: (half,)}
                src = gw.at[gwi({**at, **tail}, part)]
                send(direct, src, buf.at[bufi({**shifted, **tail}, part)], near(d, shift))

    def end(n, ring):
        arrived(rings[n][1])
        for c in range(3):
            d, nxt, at, shifted, part = flow(n, c, ring)
            spot = gwi({**at, d: own[d]}, part)
            got = bufi({**shifted, d: own[d]}, part)
            gw[spot] = (
                gw[spot].astype(F32) + r2p[got].astype(F32) + r2m[got].astype(F32)
            ).astype(BF16)

    def last_start(n):
        rings[n] = group(3, n)
        for c in range(3):
            a, b, d = ORDERS[c]
            for shift, buf in ((1, r1), (-1, r2p), (2, r2m)):
                at = {**own, a: step(a, shift)}
                to = {**at, d: step(d, 2)}
                part = piece(n, c)
                send(rings[n], gw.at[gwi(at, part)], buf.at[bufi(to, part)], near(a, shift))

    def last_end(n):
        arrived(rings[n])
        for c in range(3):
            d = ORDERS[c][2]
            part = piece(n, c)
            got = bufi({**own, d: step(d, 2)}, part)
            total = gw[gwi(own, part)].astype(F32)
            for buf in (r1, r2p, r2m):
                total = total + buf[got].astype(F32)
            gw_out[:, part] = total * (1.0 / 256.0)

    OTHERS = [(sa, sb) for sb in (2, 1, -1, 0) for sa in (2, 1, -1, 0) if (sa, sb) != (0, 0)]

    def plane_start(n):
        if n == 1:
            pl.semaphore_wait(plane_sem, len(beside))
        rings[n] = (group(12, n), group(3, n))
        for i, (sa, sb) in enumerate(OTHERS):
            for c in range(3):
                a, b, d = ORDERS[c]
                part = piece(n, c)
                src = gw.at[gwi({**own, a: step(a, sa), b: step(b, sb)}, part)]
                dst = r1.at[bufi({**own, d: step(d, 2)}, part)]
                send(rings[n][i // 12], src, dst, away({a: sa, b: sb}))

    def plane_end(n):
        arrived(rings[n][0])
        arrived(rings[n][1])
        for c in range(3):
            a, b, d = ORDERS[c]
            part = piece(n, c)
            total = gw[gwi(own, part)].astype(F32)
            for sa, sb in OTHERS:
                at = {a: step(a, sa), b: step(b, sb), d: step(d, 2)}
                total = total + r1[bufi(at, part)].astype(F32)
            gw_out[:, part] = total * (1.0 / 256.0)

    def attended_grads_part(n):
        lax.fori_loop(CHUNKS[n][0] // 256, CHUNKS[n][3] // 256, attended_grads, 0)

    def attended_grads(i, _):
        at = pl.ds(pl.multiple_of(i * 256, 256), 256)
        block = w[:, :, :, :, :, :, at].reshape(D, 256)
        att[:, at] = dot(up[...], block).astype(BF16)
        return 0

    def backward_heads(lo, hi):
        def body(i, _):
            done = []
            for j in range(2):
                h = i * 2 + j
                at = pl.ds(pl.multiple_of(h * DH, DH), DH)
                args = q[:, at], k[:, at], v[:, at], att[:, at], prob_a[h], prob_b[h]
                done.append((at, head_backward(*args)))
            for at, (dq, dk, dv) in done:
                q[:, at] = dq
                for i in range(2):
                    k[i * HALF : (i + 1) * HALF, at] = dk[i]
                    v[i * HALF : (i + 1) * HALF, at] = dv[i]
            return 0

        lax.fori_loop(lo // 2, hi // 2, body, 0)

    def loaded(trio):
        for copy in trio:
            copy.wait()

    loaded(loads[0])
    forward_pairs(0, 3)
    up_load.wait()
    weight_partial(0, 0, 1)
    gather_a(0)
    gather_a(1)
    gather_a(2)
    spread(0, (0,))
    spread(1, (0,))
    spread(2, (0,))
    weight_partial(0, 1, 2)
    swap_pair(0, 0)
    weight_partial(0, 2, 4)
    swap_pair(0, 1)
    loaded(loads[1])
    forward_pairs(3, 4)
    gather_b(0)
    spread(0, (1, -1))
    gather_b(1)
    spread(1, (1, -1))
    forward_pairs(4, 5)
    gather_b(2)
    spread(2, (1, -1))
    add_pair(0)
    forward_pairs(5, 6)
    gather_c(0)
    gather_c(1)
    weight_partial(1, 0, 2)
    swap_pair(1, 0)
    gather_c(2)
    start(0, 0)
    weight_partial(1, 2, 4)
    swap_pair(1, 1)
    gather_d(0)
    loaded(loads[2])
    forward_pairs(6, 7)
    gather_d(1)
    forward_pairs(7, 8)
    gather_d(2)
    add_pair(1)
    middle(0, 0)
    start(1, 0)
    weight_partial(2, 0, 2)
    swap_pair(2, 0)
    weight_partial(2, 2, 4)
    swap_pair(2, 1)
    gather_e(0)
    gather_e(1)
    arrived(crossed[0])
    attended_grads_part(0)
    add_pair(2)
    start(2, 0)
    gather_e(2)
    end(0, 0)
    start(0, 1)
    backward_heads(0, 4)
    middle(1, 0)
    arrived(crossed[1])
    attended_grads_part(1)
    middle(2, 0)
    middle(0, 1)
    backward_heads(4, 6)
    end(1, 0)
    plane_start(1)
    backward_heads(6, 10)
    end(2, 0)
    plane_start(2)
    end(0, 1)
    last_start(0)
    backward_heads(10, 12)
    arrived(crossed[2])
    attended_grads_part(2)
    plane_end(1)
    backward_heads(12, 16)
    last_end(0)
    plane_end(2)
    for g in range(len(groups)):
        sent(g)


GROUPS = 48


def whole(q, k, v, up, w, ids):
    chips = (RING, 2, 2, RING)
    wide = jax.ShapeDtypeStruct((LEN, HD), BF16)
    hbm_spec = pl.BlockSpec(memory_space=pltpu.HBM)
    vmem_spec = pl.BlockSpec(memory_space=pltpu.VMEM)
    return pl.pallas_call(
        kernel,
        in_specs=[hbm_spec] * 6,
        out_specs=[vmem_spec] * 4,
        out_shape=[wide] * 3 + [jax.ShapeDtypeStruct((ROWS, HD), F32)],
        scratch_shapes=[pltpu.VMEM((LEN, D), BF16), pltpu.VMEM((D, LEN), BF16)]
        + [pltpu.VMEM((*chips, 2, ROWS, HD), BF16)] * 2
        + [pltpu.VMEM((*chips, ROWS, HD), BF16)] * 4
        + [pltpu.VMEM((LEN, HD), BF16)]
        + [pltpu.VMEM((H, HALF, LEN), BF16), pltpu.VMEM((H, HALF, HALF), BF16)]
        + [pltpu.VMEM((HALF, LEN), F32), pltpu.VMEM((HALF, HALF), F32)]
        + [
            pltpu.VMEM((1, LEN), jnp.int32),
            pltpu.SemaphoreType.DMA((12,)),
            pltpu.SemaphoreType.DMA((GROUPS,)),
            pltpu.SemaphoreType.DMA((GROUPS,)),
            pltpu.SemaphoreType.REGULAR,
        ],
        compiler_params=pltpu.CompilerParams(
            collective_id=0, has_side_effects=True, vmem_limit_bytes=50_000_000
        ),
        name="whole",
    )(ids, q, k, v, up, w)


def pass_on_kernel(*refs):
    held, results, sems = refs[:4], refs[4:8], refs[8]
    copies = [
        pltpu.make_async_copy(src, dst, sems.at[i])
        for i, (src, dst) in enumerate(zip(held, results))
    ]
    for copy in copies:
        copy.start()
    for copy in copies:
        copy.wait()


def pass_on(*arrays):
    return pl.pallas_call(
        pass_on_kernel,
        in_specs=[pl.BlockSpec(memory_space=pltpu.VMEM)] * 4,
        out_specs=[pl.BlockSpec(memory_space=pltpu.HBM)] * 4,
        out_shape=[jax.ShapeDtypeStruct(a.shape, a.dtype) for a in arrays],
        scratch_shapes=[pltpu.SemaphoreType.DMA((4,))],
        compiler_params=pltpu.CompilerParams(vmem_limit_bytes=8_000_000),
        name="pass_on",
    )(*arrays)


def shards(queries, key_rows, values, upstream, out_weight, sample_ids):
    return tuple(pass_on(*whole(queries, key_rows, values, upstream, out_weight, sample_ids)))


def solution(mesh):
    return jax.shard_map(
        shards,
        mesh=mesh,
        in_specs=(P(ALL, None),) * 6,
        out_specs=(P(ALL, None),) * 4,
        check_vma=False,
    )
```

```python
import functools
import math

import jax
import jax.numpy as jnp
from jax import lax
from jax.experimental import pallas as pl
from jax.experimental.pallas import tpu as pltpu
from jax.sharding import PartitionSpec as P

H = 16
DH = 128
LEN = 512
HALF = 256
D = 2048
HD = 2048
RING = 4
ROWS = 16
SCALING = 1.0 / math.sqrt(DH)
SCALE2 = SCALING * math.log2(math.e)
NEG = -1e30
ALL = ("dp", "rep")
F32 = jnp.float32
BF16 = jnp.bfloat16
MESH = pl.DeviceIdType.MESH
EVERY = slice(None)

NN = (((1,), (0,)), ((), ()))
NT = (((1,), (1,)), ((), ()))
TN = (((0,), (0,)), ((), ()))

ORDERS = (("x", "y", "z"), ("y", "z", "x"), ("z", "x", "y"))
CHUNKS = ((0, 256, 512, 768), (768, 1024, 1280, 1536), (1536, 1664, 1792, 2048))


def dot(a, b, dims=NN):
    return lax.dot_general(a, b, dims, preferred_element_type=F32)


def fill_bias(ids, bias_a, bias_b):
    start = jnp.zeros((1, LEN), jnp.int32)
    for v in range(3):
        count = jnp.sum((ids == v).astype(jnp.int32), axis=1, keepdims=True)
        start = start + jnp.where(ids > v, count, 0)
    t = lax.broadcasted_iota(jnp.int32, (HALF, LEN), 1)
    u = lax.broadcasted_iota(jnp.int32, (HALF, LEN), 0)
    bias_a[...] = jnp.where((u >= start) & (u <= t), 0.0, NEG).astype(F32)
    t = lax.broadcasted_iota(jnp.int32, (HALF, HALF), 1) + HALF
    u = lax.broadcasted_iota(jnp.int32, (HALF, HALF), 0) + HALF
    bias_b[...] = jnp.where((u >= start[:, HALF:]) & (u <= t), 0.0, NEG).astype(F32)


def head_forward(q, k, v, bias_a, bias_b):
    xa = dot(k[:HALF], q, NT) * SCALE2 + bias_a[...]
    xb = dot(k[HALF:], q[HALF:], NT) * SCALE2 + bias_b[...]
    ma = jnp.max(xa, axis=0, keepdims=True)
    mb = jnp.maximum(ma[:, HALF:], jnp.max(xb, axis=0, keepdims=True))
    m = jnp.concatenate([ma[:, :HALF], mb], axis=1)
    ea = jnp.exp2(xa - m)
    eb = jnp.exp2(xb - mb)
    la = jnp.sum(ea, axis=0, keepdims=True)
    lb = la[:, HALF:] + jnp.sum(eb, axis=0, keepdims=True)
    inv = 1.0 / jnp.concatenate([la[:, :HALF], lb], axis=1)
    pa = (ea * inv).astype(BF16)
    pb = (eb * inv[:, HALF:]).astype(BF16)
    vt = v.T
    ot_a = dot(vt[:, :HALF], pa)
    ot_b = dot(vt[:, HALF:], pb)
    ot = jnp.concatenate([ot_a[:, :HALF], ot_a[:, HALF:] + ot_b], axis=1)
    return ot.astype(BF16).T, pa, pb


def head_backward(q, k, v, g, low_a, low_b):
    q1, g1 = q[HALF:], g[HALF:]
    dpa = dot(v[:HALF], g, NT)
    dpb = dot(v[HALF:], g1, NT)
    pa = low_a.astype(F32)
    pb = low_b.astype(F32)
    ia = jnp.sum(pa * dpa, axis=0, keepdims=True)
    ib = ia[:, HALF:] + jnp.sum(pb * dpb, axis=0, keepdims=True)
    inner = jnp.concatenate([ia[:, :HALF], ib], axis=1)
    dsa = (pa * (dpa - inner)).astype(BF16)
    dsb = (pb * (dpb - ib)).astype(BF16)
    gv = (dot(low_a, g).astype(BF16), dot(low_b, g1).astype(BF16))
    gk = ((dot(dsa, q) * SCALING).astype(BF16), (dot(dsb, q1) * SCALING).astype(BF16))
    kt = k.T
    qt_a = dot(kt[:, :HALF], dsa)
    qt_b = dot(kt[:, HALF:], dsb)
    qt = jnp.concatenate([qt_a[:, :HALF], qt_a[:, HALF:] + qt_b], axis=1)
    return (qt * SCALING).astype(BF16).T, gk, gv


def kernel(
    ids_hbm, q_hbm, k_hbm, v_hbm, up_hbm, w_hbm,
    q, k, v, gw_out,
    up, up_t, w, gw, pair, r1, r2p, r2m, att, prob_a, prob_b, bias_a, bias_b,
    ids, load_sem, send_sem, recv_sem, plane_sem,
):
    dp, rep = lax.axis_index("dp"), lax.axis_index("rep")
    core = lax.rem(rep, 2)
    own = {
        "x": dp // 2,
        "y": lax.rem(rep // 2, RING),
        "z": (rep // 8) * 2 + lax.rem(dp, 2),
    }

    def away(shifts):
        x, y, z = (lax.rem(own[d] + shifts.get(d, 0) + RING, RING) for d in ("x", "y", "z"))
        return (x * 2 + lax.rem(z, 2), (z // 2) * 8 + y * 2 + core)

    def near(dim, shift):
        return away({dim: shift})

    sibling = (dp, rep + 1 - 2 * core)

    def step(dim, shift):
        return lax.rem(own[dim] + shift + RING, RING)

    def place(at):
        x, y = (
            pl.ds(2 * i[0], 2) if isinstance(i, tuple) else i
            for i in (at.get("x", EVERY), at.get("y", EVERY))
        )
        z = at.get("z", EVERY)
        if isinstance(z, tuple):
            return (x, EVERY, z[0], y)
        if z is EVERY:
            return (x, EVERY, EVERY, y)
        return (x, lax.rem(z, 2), z // 2, y)

    def cols(lo, hi):
        return pl.ds(lo, hi - lo)

    groups = []

    def blob(k, part):
        lead = {
            3: (0, 0, 0, pl.ds(0, 3)),
            4: (0, 0, 0, EVERY),
            8: (0, 0, EVERY, EVERY),
            12: (pl.ds(0, 3), 0, 0, EVERY),
            16: (0, EVERY, EVERY, EVERY),
            32: (pl.ds(0, 2), EVERY, EVERY, EVERY),
            64: (EVERY, EVERY, EVERY, EVERY),
        }[k]
        return pair.at[(*lead, EVERY, part)]

    def group(k, n):
        groups.append(blob(k, chunk(n)))
        return len(groups) - 1

    def send(g, src, dst, device):
        pltpu.make_async_remote_copy(
            src_ref=src, dst_ref=dst, send_sem=send_sem.at[g], recv_sem=recv_sem.at[g],
            device_id=device, device_id_type=MESH,
        ).start()

    def arrived(g):
        pltpu.make_async_copy(groups[g], groups[g], recv_sem.at[g]).wait()

    def sent(g):
        pltpu.make_async_copy(groups[g], groups[g], send_sem.at[g]).wait()

    def chunk(n):
        return cols(CHUNKS[n][0], CHUNKS[n][3])

    def piece(n, c):
        return cols(CHUNKS[n][c], CHUNKS[n][c + 1])

    barrier = pltpu.get_barrier_semaphore()
    beside = [near(d, s) for d in ("x", "y", "z") for s in (1, -1, 2)]
    peers = beside + [sibling]
    for peer in peers:
        pl.semaphore_signal(barrier, inc=1, device_id=peer, device_id_type=MESH)
    here = place(own)
    w_load = pltpu.make_async_copy(w_hbm, w.at[(*here, core)], load_sem.at[0])
    w_load.start()
    ids_load = pltpu.make_async_copy(ids_hbm, ids, load_sem.at[11])
    ids_load.start()
    loads = []
    for c in range(3):
        part = cols(CHUNKS[c][0], CHUNKS[c][3])
        trio = []
        for i, (src, dst) in enumerate(((q_hbm, q), (k_hbm, k), (v_hbm, v))):
            copy = pltpu.make_async_copy(
                src.at[:, part], dst.at[:, part], load_sem.at[1 + 3 * c + i]
            )
            copy.start()
            trio.append(copy)
        loads.append(trio)
    up_load = pltpu.make_async_copy(up_hbm, up, load_sem.at[10])
    up_load.start()

    pl.semaphore_wait(barrier, len(peers))
    w_load.wait()

    def share(g, at, part, device):
        ref = w.at[(*place(at), core, EVERY, part)]
        send(g, ref, ref, device)

    crossed = [group(64, n) for n in range(3)]
    gather = {}

    def cross(n, c, at):
        share(crossed[n], at, piece(n, c), sibling)

    def gather_start(n):
        gather[n] = group(3, n)
        for c in range(3):
            a, b, d = ORDERS[c]
            for s in (1, -1, 2):
                share(gather[n], own, piece(n, c), near(a, s))

    def gather_a(n):
        arrived(gather[n])
        gather[n] = group(8, n)
        for c in range(3):
            a, b, d = ORDERS[c]
            for s in (1, -1):
                share(gather[n], {b: own[b], d: own[d]}, piece(n, c), near(b, s))

    def gather_b(n):
        arrived(gather[n])
        gather[n] = group(4, n)
        for c in range(3):
            a, b, d = ORDERS[c]
            for s, half in ((1, 0), (-1, 1)):
                at = {a: (half,), b: step(b, -s), d: own[d]}
                share(gather[n], at, piece(n, c), near(b, s))

    def gather_c(n):
        arrived(gather[n])
        spread(n, (2,))
        for c in range(3):
            d = ORDERS[c][2]
            cross(n, c, {d: own[d]})

    def gather_d(n):
        arrived(wide[n])
        gather[n] = group(16, n)
        for c in range(3):
            a, b, d = ORDERS[c]
            for s, half in ((1, 0), (-1, 1)):
                share(gather[n], {b: (half,), d: step(d, -s)}, piece(n, c), near(d, s))
        for c in range(3):
            d = ORDERS[c][2]
            for s in (1, -1):
                cross(n, c, {d: step(d, s)})

    def gather_e(n):
        arrived(gather[n])
        for c in range(3):
            d = ORDERS[c][2]
            cross(n, c, {d: step(d, 2)})

    wide = [group(32, n) for n in range(3)]

    def spread(n, shifts):
        for shift in shifts:
            for c in range(3):
                a, b, d = ORDERS[c]
                at = {b: step(b, shift), d: own[d]}
                for s in (1, -1):
                    share(wide[n], at, piece(n, c), near(d, s))

    for n in range(3):
        gather_start(n)

    for peer in beside:
        pl.semaphore_signal(plane_sem, inc=1, device_id=peer, device_id_type=MESH)

    ids_load.wait()
    fill_bias(ids[...], bias_a, bias_b)

    def forward_pairs(lo, hi):
        def body(i, _):
            done = []
            for j in range(2):
                h = i * 2 + j
                at = pl.ds(pl.multiple_of(h * DH, DH), DH)
                done.append((h, at, head_forward(q[:, at], k[:, at], v[:, at], bias_a, bias_b)))
            for h, at, (o, pa, pb) in done:
                att[:, at] = o
                prob_a[h] = pa
                prob_b[h] = pb
            return 0

        lax.fori_loop(lo, hi, body, 0)

    def weight_partial(n, lo_i, hi_i):
        lo, hi = CHUNKS[n][0], CHUNKS[n][3]

        def body(i, _):
            rows = pl.ds(pl.multiple_of(i * 512, 512), 512)
            if n == 0:
                up_t[rows, :] = up[:, rows].T
            block = dot(up_t[rows, :], att[:, lo:hi]).astype(BF16)
            gw[i, :, :, :, :, :, cols(lo, hi)] = block.reshape(2, 2, RING, 2, ROWS, hi - lo)
            return 0

        lax.fori_loop(lo_i, hi_i, body, 0)

    swaps = {}

    def swap_pair(n, half):
        g = group(32, n)
        swaps[n, half] = g
        part, x = chunk(n), pl.ds(2 * half, 2)
        send(g, gw.at[x, :, :, :, 1 - core, :, part], pair.at[x, :, :, :, :, part], sibling)

    def add_pair(n):
        part = chunk(n)

        def body(i, _):
            mine = gw[i, :, :, :, core, :, part].astype(F32)
            gw[i, :, :, :, core, :, part] = (
                mine + pair[i, :, :, :, :, part].astype(F32)
            ).astype(BF16)
            return 0

        for half in range(2):
            arrived(swaps[n, half])
            lax.fori_loop(2 * half, 2 * half + 2, body, 0)

    def gwi(at, part):
        return (*place(at), core, EVERY, part)

    def bufi(at, part):
        return (*place(at), EVERY, part)

    def flow(n, c, ring):
        a, b, d = ORDERS[c]
        if ring == 0:
            return (d, b, {}, {}, piece(n, c))
        return (b, a, {d: own[d]}, {d: step(d, 1)}, piece(n, c))

    rings = {}
    SIDES = ((1, 0, r2p), (-1, 1, r2m))

    def start(n, ring):
        relayed, direct = group(4 if ring else 16, n), group(8 if ring else 32, n)
        rings[n] = (relayed, direct)
        for c in range(3):
            d, nxt, at, shifted, part = flow(n, c, ring)
            for shift, half, buf in SIDES:
                far = {**at, d: step(d, 2), nxt: (half,)}
                send(relayed, gw.at[gwi(far, part)], r1.at[bufi(far, part)], near(d, shift))
        for c in range(3):
            d, nxt, at, shifted, part = flow(n, c, ring)
            for shift, half, buf in SIDES:
                tail = {d: step(d, shift), nxt: (1 - half,)}
                src = gw.at[gwi({**at, **tail}, part)]
                send(direct, src, buf.at[bufi({**shifted, **tail}, part)], near(d, shift))

    def middle(n, ring):
        relayed, direct = rings[n]
        arrived(relayed)
        for c in range(3):
            d, nxt, at, shifted, part = flow(n, c, ring)
            for shift, half, buf in SIDES:
                tail = {d: step(d, shift), nxt: (half,)}
                src = gwi({**at, **tail}, part)
                gw[src] = (
                    gw[src].astype(F32) + r1[bufi({**at, **tail}, part)].astype(F32)
                ).astype(BF16)
        for c in range(3):
            d, nxt, at, shifted, part = flow(n, c, ring)
            for shift, half, buf in SIDES:
                tail = {d: step(d, shift), nxt: (half,)}
                src = gw.at[gwi({**at, **tail}, part)]
                send(direct, src, buf.at[bufi({**shifted, **tail}, part)], near(d, shift))

    def end(n, ring):
        arrived(rings[n][1])
        for c in range(3):
            d, nxt, at, shifted, part = flow(n, c, ring)
            spot = gwi({**at, d: own[d]}, part)
            got = bufi({**shifted, d: own[d]}, part)
            gw[spot] = (
                gw[spot].astype(F32) + r2p[got].astype(F32) + r2m[got].astype(F32)
            ).astype(BF16)

    def last_start(n):
        rings[n] = group(3, n)
        for c in range(3):
            a, b, d = ORDERS[c]
            for shift, buf in ((1, r1), (-1, r2p), (2, r2m)):
                at = {**own, a: step(a, shift)}
                to = {**at, d: step(d, 2)}
                part = piece(n, c)
                send(rings[n], gw.at[gwi(at, part)], buf.at[bufi(to, part)], near(a, shift))

    def last_end(n):
        arrived(rings[n])
        for c in range(3):
            d = ORDERS[c][2]
            part = piece(n, c)
            got = bufi({**own, d: step(d, 2)}, part)
            total = gw[gwi(own, part)].astype(F32)
            for buf in (r1, r2p, r2m):
                total = total + buf[got].astype(F32)
            gw_out[:, part] = total * (1.0 / 256.0)

    OTHERS = [(sa, sb) for sb in (2, 1, -1, 0) for sa in (2, 1, -1, 0) if (sa, sb) != (0, 0)]

    def plane_start(n):
        if n == 1:
            pl.semaphore_wait(plane_sem, len(beside))
        rings[n] = (group(12, n), group(3, n))
        for i, (sa, sb) in enumerate(OTHERS):
            for c in range(3):
                a, b, d = ORDERS[c]
                part = piece(n, c)
                src = gw.at[gwi({**own, a: step(a, sa), b: step(b, sb)}, part)]
                dst = r1.at[bufi({**own, d: step(d, 2)}, part)]
                send(rings[n][i // 12], src, dst, away({a: sa, b: sb}))

    def plane_end(n):
        arrived(rings[n][0])
        arrived(rings[n][1])
        for c in range(3):
            a, b, d = ORDERS[c]
            part = piece(n, c)
            total = gw[gwi(own, part)].astype(F32)
            for sa, sb in OTHERS:
                at = {a: step(a, sa), b: step(b, sb), d: step(d, 2)}
                total = total + r1[bufi(at, part)].astype(F32)
            gw_out[:, part] = total * (1.0 / 256.0)

    def attended_grads_part(n):
        lax.fori_loop(CHUNKS[n][0] // 256, CHUNKS[n][3] // 256, attended_grads, 0)

    def attended_grads(i, _):
        at = pl.ds(pl.multiple_of(i * 256, 256), 256)
        block = w[:, :, :, :, :, :, at].reshape(D, 256)
        att[:, at] = dot(up[...], block).astype(BF16)
        return 0

    def backward_heads(lo, hi):
        def body(i, _):
            done = []
            for j in range(2):
                h = i * 2 + j
                at = pl.ds(pl.multiple_of(h * DH, DH), DH)
                args = q[:, at], k[:, at], v[:, at], att[:, at], prob_a[h], prob_b[h]
                done.append((at, head_backward(*args)))
            for at, (dq, dk, dv) in done:
                q[:, at] = dq
                for i in range(2):
                    k[i * HALF : (i + 1) * HALF, at] = dk[i]
                    v[i * HALF : (i + 1) * HALF, at] = dv[i]
            return 0

        lax.fori_loop(lo // 2, hi // 2, body, 0)

    def loaded(trio):
        for copy in trio:
            copy.wait()

    loaded(loads[0])
    forward_pairs(0, 3)
    up_load.wait()
    weight_partial(0, 0, 1)
    gather_a(0)
    gather_a(1)
    gather_a(2)
    spread(0, (0,))
    spread(1, (0,))
    spread(2, (0,))
    weight_partial(0, 1, 2)
    swap_pair(0, 0)
    weight_partial(0, 2, 4)
    swap_pair(0, 1)
    loaded(loads[1])
    forward_pairs(3, 4)
    gather_b(0)
    spread(0, (1, -1))
    gather_b(1)
    spread(1, (1, -1))
    forward_pairs(4, 5)
    gather_b(2)
    spread(2, (1, -1))
    add_pair(0)
    forward_pairs(5, 6)
    gather_c(0)
    gather_c(1)
    weight_partial(1, 0, 2)
    swap_pair(1, 0)
    gather_c(2)
    start(0, 0)
    weight_partial(1, 2, 4)
    swap_pair(1, 1)
    gather_d(0)
    loaded(loads[2])
    forward_pairs(6, 7)
    gather_d(1)
    forward_pairs(7, 8)
    gather_d(2)
    add_pair(1)
    middle(0, 0)
    start(1, 0)
    weight_partial(2, 0, 2)
    swap_pair(2, 0)
    weight_partial(2, 2, 4)
    swap_pair(2, 1)
    gather_e(0)
    arrived(crossed[0])
    attended_grads_part(0)
    gather_e(1)
    add_pair(2)
    start(2, 0)
    gather_e(2)
    end(0, 0)
    start(0, 1)
    backward_heads(0, 4)
    middle(1, 0)
    arrived(crossed[1])
    attended_grads_part(1)
    middle(2, 0)
    middle(0, 1)
    backward_heads(4, 6)
    backward_heads(6, 8)
    end(1, 0)
    plane_start(1)
    backward_heads(8, 10)
    end(2, 0)
    plane_start(2)
    end(0, 1)
    last_start(0)
    backward_heads(10, 12)
    arrived(crossed[2])
    attended_grads_part(2)
    backward_heads(12, 16)
    plane_end(1)
    last_end(0)
    plane_end(2)
    for g in range(len(groups)):
        sent(g)


GROUPS = 48


def whole(q, k, v, up, w, ids):
    chips = (RING, 2, 2, RING)
    wide = jax.ShapeDtypeStruct((LEN, HD), BF16)
    hbm_spec = pl.BlockSpec(memory_space=pltpu.HBM)
    vmem_spec = pl.BlockSpec(memory_space=pltpu.VMEM)
    return pl.pallas_call(
        kernel,
        in_specs=[hbm_spec] * 6,
        out_specs=[vmem_spec] * 4,
        out_shape=[wide] * 3 + [jax.ShapeDtypeStruct((ROWS, HD), F32)],
        scratch_shapes=[pltpu.VMEM((LEN, D), BF16), pltpu.VMEM((D, LEN), BF16)]
        + [pltpu.VMEM((*chips, 2, ROWS, HD), BF16)] * 2
        + [pltpu.VMEM((*chips, ROWS, HD), BF16)] * 4
        + [pltpu.VMEM((LEN, HD), BF16)]
        + [pltpu.VMEM((H, HALF, LEN), BF16), pltpu.VMEM((H, HALF, HALF), BF16)]
        + [pltpu.VMEM((HALF, LEN), F32), pltpu.VMEM((HALF, HALF), F32)]
        + [
            pltpu.VMEM((1, LEN), jnp.int32),
            pltpu.SemaphoreType.DMA((12,)),
            pltpu.SemaphoreType.DMA((GROUPS,)),
            pltpu.SemaphoreType.DMA((GROUPS,)),
            pltpu.SemaphoreType.REGULAR,
        ],
        compiler_params=pltpu.CompilerParams(
            collective_id=0, has_side_effects=True, vmem_limit_bytes=50_000_000
        ),
        name="whole",
    )(ids, q, k, v, up, w)


def pass_on_kernel(*refs):
    held, results, sems = refs[:4], refs[4:8], refs[8]
    copies = [
        pltpu.make_async_copy(src, dst, sems.at[i])
        for i, (src, dst) in enumerate(zip(held, results))
    ]
    for copy in copies:
        copy.start()
    for copy in copies:
        copy.wait()


def pass_on(*arrays):
    return pl.pallas_call(
        pass_on_kernel,
        in_specs=[pl.BlockSpec(memory_space=pltpu.VMEM)] * 4,
        out_specs=[pl.BlockSpec(memory_space=pltpu.HBM)] * 4,
        out_shape=[jax.ShapeDtypeStruct(a.shape, a.dtype) for a in arrays],
        scratch_shapes=[pltpu.SemaphoreType.DMA((4,))],
        compiler_params=pltpu.CompilerParams(vmem_limit_bytes=8_000_000),
        name="pass_on",
    )(*arrays)


def shards(queries, key_rows, values, upstream, out_weight, sample_ids):
    return tuple(pass_on(*whole(queries, key_rows, values, upstream, out_weight, sample_ids)))


def solution(mesh):
    return jax.shard_map(
        shards,
        mesh=mesh,
        in_specs=(P(ALL, None),) * 6,
        out_specs=(P(ALL, None),) * 4,
        check_vma=False,
    )
```
